256 devices in a mesh: grp: 64 (over y, x, z_lo, core), blk: 4 (over z_hi).
Axes of the slice: x: 4, y: 4, z: 8 (z_hi: 4, z_lo: 2; z = z_hi * 2 + z_lo), core: 2. Of those that a mesh axis runs over, the one named last changes fastest.
Arguments:
- tokens: bfloat16 [2048, 6144], P(('grp', 'blk')), may hold values from -6 to 6
- norm_gain: bfloat16 [6144], replicated, may hold values from 0.099609375 to 1.8984375
- expert_ids: int32 [2048, 2], P(('grp', 'blk')), may hold values from 0 to 7, all different within a row; in each aligned block of 8 rows (0 to 7, 8 to 15, ...) at most 3 rows name the same one
- combine: float32 [2048, 2], P(('grp', 'blk')), may hold values from 0.2 to 1
- w_gate: bfloat16 [6144, 65536], P(None, ('grp', 'blk')), may hold values from -0.078125 to 0.078125
- w_up: bfloat16 [6144, 65536], P(None, ('grp', 'blk')), may hold values from -0.078125 to 0.078125
- w_down: bfloat16 [65536, 6144], P(('grp', 'blk')), may hold values from -0.0625 to 0.0625
Outputs:
- layer_out: bfloat16 [2048, 6144], P(('grp', 'blk'))
The draws below stay inside these ranges and needn't reach their ends.
Inputs may be any that keep to these rules, and one draw needn't show every extreme that they name: `expert_ids`: each row names 2 different experts; in the rows of one device no expert is named more than 3 times, a bound that some block reaches.
All inputs are finite; a program needn't handle non-finite values.
Results may differ from the reference program's by a relative error of at most 0.0075.
Values may be sent and summed in bfloat16 or wider, within the bound.
A program may use at most 128 MiB of HBM per device.

```python
import math
import jax
import jax.numpy as jnp
import numpy as np
from jax import lax

D = 6144
FF = 8192
E = 8
TOP = 2
TOK_DEV = 8
CAP = 3
TOKENS = 2048
N_GRP = 64
N_BLK = 4


def steps_of(stream_key, shape, shards, smallest, largest):
    def one(axis_at, shards_of):
        steps = jax.random.uniform(jax.random.fold_in(jax.random.fold_in(stream_key, 6), axis_at), (shards_of,), jnp.float32, smallest / len(shards), largest / len(shards))
        return jnp.repeat(jnp.exp(steps), shape[axis_at] // shards_of).reshape((-1,) + (1,) * (len(shape) - axis_at - 1))

    loudness = one(*shards[0])
    for cut in shards[1:]:
        loudness = loudness * one(*cut)
    return loudness


def routed_block(rng, own, number, rows, number_of, top, reach, skew):
    ranking = jax.random.permutation(rng, number_of)
    packed, usual = shares(number_of, rows * top, reach, skew, True), shares(number_of, rows * top, reach, skew, False)
    places = jnp.arange(number_of)

    def named(lengths, turn):
        used = int((lengths > 0).sum())
        fixed = max(1, used // 4)
        passed = fixed + (places - fixed + turn * (used - fixed)) % max(1, number_of - fixed)
        return jnp.zeros((number_of,), jnp.int32).at[ranking[jnp.where(places < fixed, places, passed)]].set(jnp.asarray(lengths, jnp.int32))

    lengths = jnp.where(number % 4 == 0, named(packed, number // 4), named(usual, number - number // 4 - 1))
    mixed = jax.random.permutation(jax.random.fold_in(own, 3), number_of)
    source_of, receiver = mixed[0:number_of // 2 * 2:2], mixed[1:number_of // 2 * 2:2]
    margin = jnp.minimum(lengths[source_of] - 1, reach - lengths[receiver]) // 2
    margin = jnp.where((source_of == ranking[0]) | (receiver == ranking[0]) | (lengths[receiver] == 0), 0, jnp.maximum(margin, 0))
    passed = jax.random.randint(jax.random.fold_in(own, 4), (number_of // 2,), 0, 1 << 20) % (margin + 1)
    lengths = lengths.at[source_of].add(-passed).at[receiver].add(passed)
    items = jnp.searchsorted(jnp.cumsum(lengths), jnp.arange(rows * top), side="right").astype(jnp.int32)
    listing = items.reshape(top, rows).T
    listing = listing[jax.random.permutation(jax.random.fold_in(own, 1), rows)]
    turn = jax.random.randint(jax.random.fold_in(own, 2), (rows, 1), 0, top)
    return jnp.take_along_axis(listing, (jnp.arange(top)[None, :] + turn) % top, axis=1)


def shares(amount, total, reach, lean, full):
    portions = [(1 << 20) // math.isqrt(rank ** lean) + 1 for rank in range(1, amount + 1)]
    largest = reach if full else min(reach, max(-(-total // amount), total * portions[0] // sum(portions)))
    least = 1 if total - largest >= amount - 1 else 0
    counts, rest = [largest] + [least] * (amount - 1), total - largest - least * (amount - 1)
    while rest > 0:
        candidates = [i for i in range(1, amount) if counts[i] < largest] or [i for i in range(1, amount) if counts[i] < reach]
        whole, left = sum([portions[i] for i in candidates]), rest
        for i in candidates:
            extra = min(reach - counts[i], max(1, left * portions[i] // whole), rest)
            counts[i] = counts[i] + extra
            rest = rest - extra
    return np.array(counts)


def gaussian(rng, shape, width, bound, split=(), kind=jnp.bfloat16):
    factor_of = steps_of(rng, shape, split, -0.22, 0.18) if split else 1.0
    entries = jax.random.normal(rng, shape, jnp.float32) * width * factor_of
    return jnp.minimum(jnp.maximum(entries, -bound), bound).astype(kind)


def setup_inputs(seed: int = 0) -> dict:
    keys = jax.random.split(jax.random.key(seed), 8)
    tokens = gaussian(keys[0], (TOKENS, D), 1.0, 6.0, ((0, 256),))
    norm_gain = jnp.clip(1.0 + 0.18 * jax.random.normal(keys[1], (D,), jnp.float32), 0.099609375, 1.8984375).astype(jnp.bfloat16)
    expert_ids_keys = jax.random.split(jax.random.fold_in(keys[2], 1), TOKENS // TOK_DEV)
    expert_ids_turns = jax.random.permutation(jax.random.fold_in(keys[2], 3), TOKENS // TOK_DEV)
    expert_ids = jax.vmap(lambda own, number: routed_block(jax.random.fold_in(keys[2], 2), own, number, TOK_DEV, E, TOP, CAP, 2))(expert_ids_keys, expert_ids_turns).reshape((TOKENS, TOP))
    combine = jnp.clip(jnp.exp(math.log(1.0) - 1.609438 * jax.random.uniform(keys[3], (TOKENS, TOP), jnp.float32) ** steps_of(keys[3], (TOKENS, TOP), ((0, 256),), -0.2, 0.2)), 0.2, 1.0)
    w_gate = gaussian(keys[4], (D, E * FF), D ** -0.5, 0.078125, ((1, 256),))
    w_up = gaussian(keys[5], (D, E * FF), D ** -0.5, 0.078125, ((1, 256),))
    w_down = gaussian(keys[6], (E * FF, D), FF ** -0.5, 0.0625, ((0, 256),))
    return {"tokens": tokens, "norm_gain": norm_gain, "expert_ids": expert_ids, "combine": combine, "w_gate": w_gate, "w_up": w_up, "w_down": w_down}


epsilon = 1e-05

def reference(tokens, norm_gain, expert_ids, combine, w_gate, w_up, w_down):
    blocks = TOKENS // TOK_DEV
    pair_count = TOKENS * TOP
    per_block = TOK_DEV * TOP
    wide_tokens = tokens.astype(jnp.float32)
    scale_rows = lax.rsqrt(lax.optimization_barrier(jnp.mean(wide_tokens * wide_tokens, axis=1, keepdims=True)) + epsilon)
    normed = (wide_tokens * scale_rows * norm_gain.astype(jnp.float32)[None, :]).astype(jnp.bfloat16)
    pair_rows = jnp.repeat(normed, TOP, axis=0)
    block_ids = expert_ids.reshape(blocks, per_block)
    one_hot = (block_ids[:, :, None] == jnp.arange(E, dtype=jnp.int32)[None, None, :]).astype(jnp.int32)
    earlier = jnp.cumsum(one_hot, axis=1) - one_hot
    slot_index = lax.optimization_barrier(jnp.sum(earlier * one_hot, axis=2))
    global_slot = (slot_index + CAP * jnp.arange(blocks, dtype=jnp.int32)[:, None]).reshape(pair_count).astype(jnp.int32)
    route_ids = expert_ids.reshape(pair_count).astype(jnp.int32)
    slot_table = jnp.zeros((E, blocks * CAP), jnp.int32).at[route_ids, global_slot].set(jnp.arange(pair_count, dtype=jnp.int32))
    unit_count = E * FF // (N_GRP * N_BLK)

    def one_expert(expert_index):
        chosen = pair_rows[slot_table[expert_index]]
        gate_cols = lax.dynamic_slice_in_dim(w_gate, expert_index * FF, FF, 1)
        up_cols = lax.dynamic_slice_in_dim(w_up, expert_index * FF, FF, 1)
        down_rows = lax.dynamic_slice_in_dim(w_down, expert_index * FF, FF, 0)
        gate_val = jnp.dot(chosen, gate_cols, preferred_element_type=jnp.float32)
        up_val = jnp.dot(chosen, up_cols, preferred_element_type=jnp.float32)
        hidden = (jax.nn.silu(gate_val) * up_val).astype(jnp.bfloat16)

        def add_block(block_index, running):
            start = (block_index * unit_count).astype(jnp.int32)
            partial_value = jnp.dot(lax.dynamic_slice_in_dim(hidden, start, unit_count, 1), lax.dynamic_slice_in_dim(down_rows, start, unit_count, 0), preferred_element_type=jnp.float32)
            rounded = lax.optimization_barrier(partial_value.astype(jnp.bfloat16))
            return running + rounded.astype(jnp.float32)
        return lax.fori_loop(0, FF // unit_count, add_block, jnp.zeros((blocks * CAP, D), jnp.float32))
    outputs = lax.map(one_expert, jnp.arange(E, dtype=jnp.int32))
    pair_out = outputs[route_ids, global_slot]
    expert_mix = lax.optimization_barrier(jnp.sum(pair_out.reshape(TOKENS, TOP, D) * combine[:, :, None], axis=1))
    return (wide_tokens + expert_mix).astype(jnp.bfloat16)
```

```python
import jax
import jax.numpy as jnp
from jax import lax
from jax.experimental import pallas as pl
from jax.experimental.pallas import tpu as pltpu
from jax.sharding import PartitionSpec as P

MESH = pl.DeviceIdType.MESH
D = 6144
HID = 256
QW = D // 4
BLK = 48
EPS = 1e-05
BF = jnp.bfloat16
F32 = jnp.float32


def dot(a, b):
    return jnp.dot(a, b, preferred_element_type=F32)


def iota(shape, dim):
    return lax.broadcasted_iota(jnp.int32, shape, dim)


def kernel(
    tok_ref,
    gain_ref,
    ids_ref,
    comb_ref,
    wg_hbm,
    wu_hbm,
    wd_hbm,
    out_ref,
    wg,
    wu,
    wd,
    sb,
    arr,
    xs,
    ys,
    hid,
    rz,
    rp,
    sums,
    ex,
    home,
    send_sem,
    recv_sem,
    local_sem,
):
    grp = lax.axis_index("grp")
    blk = lax.axis_index("blk")
    core = lax.rem(grp, 2)
    mz = blk * 2 + lax.rem(lax.div(grp, 2), 2)
    mx = lax.rem(lax.div(grp, 4), 4)
    my = lax.div(grp, 16)
    yx = my * 4 + mx
    par = lax.rem(mx, 2)

    def dev(y, x, z, c):
        return (((y * 4 + x) * 2 + lax.rem(z, 2)) * 2 + c, lax.div(z, 2))

    def expert_at(y, x):
        return y * 2 + lax.div(x, 2)

    up = dev(my, mx, lax.rem(mz + 1, 8), core)
    down = dev(my, mx, lax.rem(mz + 7, 8), core)
    pair = dev(my, mx + 1 - 2 * par, mz, core)
    twin = dev(my, mx, mz, 1 - core)
    plane = []
    for d in range(1, 16):
        ty = lax.rem(my + d // 4, 4)
        tx = lax.rem(mx + d % 4, 4)
        plane.append((d, ty, tx))

    barrier = pltpu.get_barrier_semaphore()
    for target in [dev(ty, tx, mz, core) for _, ty, tx in plane] + [up, down, twin]:
        pl.semaphore_signal(barrier, inc=1, device_id=target, device_id_type=MESH)

    local = [
        pltpu.make_async_copy(wg_hbm, wg.at[0], local_sem.at[0]),
        pltpu.make_async_copy(wu_hbm, wu.at[0], local_sem.at[1]),
        pltpu.make_async_copy(wd_hbm, wd.at[pl.ds(0, HID), :], local_sem.at[2]),
    ]
    for copy in local:
        copy.start()

    wide = tok_ref[...].astype(F32)
    scale = lax.rsqrt(jnp.mean(wide * wide, axis=1, keepdims=True) + EPS)
    normed = (wide * scale * gain_ref[...].astype(F32)).astype(BF).astype(F32)
    id0, id1 = ids_ref[:, 0:1], ids_ref[:, 1:2]
    tri = (iota((8, 8), 1) < iota((8, 8), 0)).astype(F32)

    def slots(expert):
        match = ((id0 == expert) | (id1 == expert)).astype(F32)
        return match, dot(tri, match)

    lane = iota((8, 128), 1)
    match, slot = slots(lane >> 4)
    chosen = (match > 0.5) & (slot.astype(jnp.int32) == (lane & 3))
    folded = jnp.zeros((128, QW), F32)
    for q in range(4):
        pick = jnp.where(chosen & (((lane >> 2) & 3) == q), 1.0, 0.0).astype(F32)
        folded += lax.dot_general(
            pick,
            normed[:, q * QW : (q + 1) * QW],
            (((0,), (0,)), ((), ())),
            preferred_element_type=F32,
        )
    sb[...] = folded.astype(BF)
    own_e = pl.multiple_of(expert_at(my, mx) * 16, 16)
    own_j = pl.multiple_of(yx * 16, 16)
    arr[pl.ds(own_j, 16), :] = sb[pl.ds(own_e, 16), :]

    pl.semaphore_wait(barrier, 18)

    sent = []
    counter = [0]

    def remote(src, dst, target, number):
        return pltpu.make_async_remote_copy(
            src_ref=src,
            dst_ref=dst,
            send_sem=send_sem.at[number],
            recv_sem=recv_sem.at[number],
            device_id=target,
            device_id_type=MESH,
        )

    def send(src, dst, target):
        copy = remote(src, dst, target, counter[0])
        counter[0] += 1
        copy.start()
        sent.append(copy)
        return copy

    def rows16(j):
        return pl.ds(pl.multiple_of(j * 16, 16), 16)

    def plane_exchange(source, landing, row_of):
        waits = []
        for d, ty, tx in plane:
            number = counter[0]
            target = dev(ty, tx, mz, core)
            send(source.at[rows16(row_of(ty, tx)), :], landing.at[rows16(yx), :], target)
            fy = lax.rem(my + 4 - d // 4, 4)
            fx = lax.rem(mx + 4 - d % 4, 4)
            waits.append(
                remote(
                    source.at[rows16(row_of(fy, fx)), :],
                    landing.at[rows16(fy * 4 + fx), :],
                    dev(fy, fx, mz, core),
                    number,
                )
            )
        return waits

    scatter = plane_exchange(sb, arr, expert_at)
    weights = [
        send(wg_hbm, wg.at[1], twin),
        send(wu_hbm, wu.at[1], twin),
        send(wd_hbm, wd.at[pl.ds(HID, HID), :], twin),
    ]
    for copy in scatter:
        copy.wait_recv()

    def plane_row(r):
        part = r >> 4
        return (r & 15) + jnp.where(
            part == 0, 0, jnp.where(part == 1, 16 * (1 + par), 16 * (2 - par))
        )

    def fold_mask(row, lane, q):
        c = lane & 3
        return (c < 3) & (((lane >> 2) & 3) == q) & ((lane >> 4) * 3 + c == plane_row(row))

    for q in range(4):
        keep = fold_mask(iota((BLK, 256), 0), iota((BLK, 256), 1), q)
        pick = jnp.where(keep, 1.0, 0.0).astype(BF)
        xs[0:BLK, q * QW : (q + 1) * QW] = dot(pick, arr[...]).astype(BF)

    def part(b, k, count=1):
        return pl.ds(b * BLK + 16 * k, 16 * count)

    def compute(start, rows):
        def gate_up(h, _):
            block = xs[start : start + rows, :]
            gate = dot(block, wg[h])
            upv = dot(block, wu[h])
            value = gate / (1.0 + jnp.exp(-gate)) * upv
            hid[0:rows, pl.ds(pl.multiple_of(h * HID, HID), HID)] = value.astype(BF)
            return 0

        lax.fori_loop(0, 2, gate_up, 0)

        def down_proj(n, _):
            cols = pl.ds(pl.multiple_of(n * 512, 512), 512)
            ys[start : start + rows, cols] = dot(hid[0:rows, :], wd[:, cols]).astype(BF)
            return 0

        lax.fori_loop(0, D // 512, down_proj, 0)

    def z_send(src_b, k, direction, dst_b):
        return send(
            xs.at[part(src_b, k), :], xs.at[part(dst_b, k), :], up if direction else down
        )

    def to_pair(b):
        return send(xs.at[part(b, 1), :], xs.at[part(b, 2), :], pair)

    arriving = {}
    for k in (1, 0):
        arriving[(1, k)] = z_send(0, k, 1, 1)
        arriving[(2, k)] = z_send(0, k, 0, 2)
    theirs = {}
    for copy in local:
        copy.wait()
    for copy in weights:
        copy.wait_recv()
    compute(0, BLK)
    for s in range(1, 5):
        for k in (1, 0):
            for direction in (1, 0):
                b = 2 * s - direction if s < 4 else 7
                if s == 4 and k == direction:
                    continue
                arriving[(b, k)].wait_recv()
                if s < 3:
                    arriving[(b + 2, k)] = z_send(b, k, direction, b + 2)
                elif s == 3 and k != direction:
                    arriving[(7, k)] = z_send(b, k, direction, 7)
                if k == 1:
                    theirs[b] = to_pair(b)
        if s > 1:
            theirs[2 * s - 3].wait_recv()
            theirs[2 * s - 2].wait_recv()
            compute(BLK * (2 * s - 3), 2 * BLK)

    partner_sum = {}

    def give_pair(b):
        partner_sum[b] = send(ys.at[part(b, 2), :], rp.at[pl.ds((b - 1) * 16, 16), :], pair)

    def rz_rows(slot, k):
        return pl.ds(slot * 32 + 16 * k, 16)

    chain = {}

    def pass_on(b, k, direction):
        terms = [ys.at[part(b, k), :]]
        if (b, k) in chain:
            chain[(b, k)].wait_recv()
            terms.append(rz.at[rz_rows(b - 1, k), :])
        if k == 1:
            partner_sum[b].wait_recv()
            terms.append(rp.at[pl.ds((b - 1) * 16, 16), :])
        if len(terms) > 1:
            add_into(ys.at[part(b, k), :], terms)
        if b == 7:
            nxt = 6 if direction else 5
        else:
            nxt = b - 2
        slot = nxt - 1 if nxt > 0 else 6 + direction
        copy = send(
            ys.at[part(b, k), :], rz.at[rz_rows(slot, k), :], up if direction else down
        )
        chain[(nxt if nxt > 0 else ("own", direction), k)] = copy

    def add_into(dst, terms):
        def body(n, _):
            cols = pl.ds(pl.multiple_of(n * 1024, 1024), 1024)
            total = terms[0][:, cols].astype(F32)
            for term in terms[1:]:
                total += term[:, cols].astype(F32)
            dst[:, cols] = total.astype(BF)
            return 0

        lax.fori_loop(0, D // 1024, body, 0)

    give_pair(5)
    give_pair(6)
    pass_on(6, 0, 1)
    theirs[7].wait_recv()
    compute(BLK * 7, BLK)
    give_pair(7)
    pass_on(7, 0, 0)
    for b in (3, 4, 1, 2):
        give_pair(b)
    pass_on(5, 1, 0)
    pass_on(7, 1, 1)
    pass_on(3, 1, 0)
    pass_on(4, 0, 1)
    pass_on(5, 0, 0)
    pass_on(6, 1, 1)
    pass_on(1, 1, 0)
    pass_on(2, 0, 1)
    pass_on(3, 0, 0)
    pass_on(4, 1, 1)
    pass_on(1, 0, 0)
    pass_on(2, 1, 1)
    for k in (0, 1):
        for direction in (0, 1):
            chain[(("own", direction), k)].wait_recv()
        add_into(
            sums.at[pl.ds(16 * k, 16), :],
            [
                ys.at[part(0, k), :],
                rz.at[rz_rows(6, k), :],
                rz.at[rz_rows(7, k), :],
            ],
        )
    sums[32:48, :] = ys[32:48, :]

    expanded = jnp.zeros((256, QW), F32)
    for q in range(4):
        keep = fold_mask(iota((256, BLK), 1), iota((256, BLK), 0), q)
        pick = jnp.where(keep, 1.0, 0.0).astype(BF)
        expanded += dot(pick, sums[:, q * QW : (q + 1) * QW])
    ex[...] = expanded.astype(BF)
    home[pl.ds(own_j, 16), :] = ex[pl.ds(own_j, 16), :]
    back = plane_exchange(ex, home, lambda y, x: y * 4 + x)

    lane = iota((8, 256), 1)
    source = lane >> 4
    expert = (source >> 2) * 2 + ((source & 3) >> 1)
    match, slot = slots(expert)
    weight = jnp.where(id0 == expert, comb_ref[:, 0:1], 0.0) + jnp.where(
        id1 == expert, comb_ref[:, 1:2], 0.0
    )
    chosen = (match > 0.5) & (slot.astype(jnp.int32) == (lane & 3))
    weight = jnp.where(chosen, weight, 0.0)
    high = weight.astype(BF).astype(F32)
    mid = (weight - high).astype(BF).astype(F32)
    low = weight - high - mid
    pieces = jnp.concatenate([high, mid, low], axis=0)
    quarter = (iota((24, 256), 1) >> 2) & 3
    for copy in back:
        copy.wait_recv()
    for q in range(4):
        cols = slice(q * QW, (q + 1) * QW)
        mix = dot(jnp.where(quarter == q, pieces, 0.0).astype(BF), home[...])
        total = mix[0:8] + mix[8:16] + mix[16:24]
        out_ref[:, cols] = (tok_ref[:, cols].astype(F32) + total).astype(BF)
    for copy in sent:
        copy.wait_send()


def on_device(tokens, norm_gain, expert_ids, combine, w_gate, w_up, w_down):
    vmem = pl.BlockSpec(memory_space=pltpu.VMEM)
    hbm = pl.BlockSpec(memory_space=pl.ANY)
    return pl.pallas_call(
        kernel,
        out_shape=jax.ShapeDtypeStruct((8, D), BF),
        in_specs=[vmem] * 4 + [hbm] * 3,
        out_specs=vmem,
        scratch_shapes=[
            pltpu.VMEM((2, D, HID), BF),
            pltpu.VMEM((2, D, HID), BF),
            pltpu.VMEM((2 * HID, D), BF),
            pltpu.VMEM((128, QW), BF),
            pltpu.VMEM((256, QW), BF),
            pltpu.VMEM((8 * BLK, D), BF),
            pltpu.VMEM((8 * BLK, D), BF),
            pltpu.VMEM((2 * BLK, 2 * HID), BF),
            pltpu.VMEM((8 * 32, D), BF),
            pltpu.VMEM((7 * 16, D), BF),
            pltpu.VMEM((BLK, D), BF),
            pltpu.VMEM((256, QW), BF),
            pltpu.VMEM((256, QW), BF),
            pltpu.SemaphoreType.DMA((75,)),
            pltpu.SemaphoreType.DMA((75,)),
            pltpu.SemaphoreType.DMA((3,)),
        ],
        compiler_params=pltpu.CompilerParams(
            collective_id=0, has_side_effects=True, vmem_limit_bytes=60 * 1024 * 1024
        ),
        name="moe",
    )(tokens, norm_gain.reshape(1, D), expert_ids, combine, w_gate, w_up, w_down)


def solution(mesh):
    return jax.shard_map(
        on_device,
        mesh=mesh,
        in_specs=(
            P(("grp", "blk"), None),
            P(),
            P(("grp", "blk"), None),
            P(("grp", "blk"), None),
            P(None, ("grp", "blk")),
            P(None, ("grp", "blk")),
            P(("grp", "blk"), None),
        ),
        out_specs=P(("grp", "blk"), None),
        check_vma=False,
    )
```
